256 devices in a mesh: actor: 32 (over z, x), mp: 8 (over y, core).
Axes of the slice: x: 4, y: 4, z: 8, core: 2. Of those that a mesh axis runs over, the one named last changes fastest.
Arguments:
- resid: bfloat16 [32768, 4096], P('actor')
- norm_gain: bfloat16 [4096], replicated, may hold values from 0.25 to 1.75
- query_weight: bfloat16 [4096, 4096], P(None, 'mp'), may hold values from -0.09375 to 0.09375
- cotangent: bfloat16 [32768, 4096], P('actor', 'mp'), may hold values from -1.25 to 1.25
- lengths: int32 [128], P('actor'), may hold values from 1 to 256
- owner: int32 [32], replicated, may hold values from 0 to 31, each once
- adapter_table: float32 [8, 32, 16, 128], P('mp', 'actor')
- moment_one: float32 [8, 32, 16, 128], P('mp', 'actor'), may hold values from -3 to 3
- moment_two: float32 [8, 32, 16, 128], P('mp', 'actor'), may hold values from 0.003 to 0.1
Outputs:
- query: bfloat16 [32768, 4096], P('actor', 'mp')
- adapter_new: float32 [8, 32, 16, 128], P('mp', 'actor')
- moment_one_new: float32 [8, 32, 16, 128], P('mp', 'actor')
- moment_two_new: float32 [8, 32, 16, 128], P('mp', 'actor')
- merged: bfloat16 [4096, 4096], P('actor', 'mp')
The draws below stay inside these ranges and needn't reach their ends.
Inputs may be any that keep to these rules, and one draw needn't show every extreme that they name: owner is a permutation: every actor keeps exactly one block of each feature slice.
All inputs are finite; a program needn't handle non-finite values.
Results may differ from the reference program's by a relative error of at most 0.0064.
Values may be sent and summed in bfloat16 or wider, within the bound.
No kernel may reach another device: no remote copies, remote signals or barrier semaphores. Data moves between devices by JAX's collectives and lax.ppermute only.
A program may use at most 128 MiB of HBM per device.

```python
import math
import jax
import jax.numpy as jnp
from jax import lax

D = 4096
R = 64
LEN = 256
TOKENS = 32768
NSEQ = 128
BLK = 16
N_ACTOR = 32
N_MP = 8


def draw_resid(key, part):
    key_base = jax.random.fold_in(key, 11)
    key_rows = jax.random.fold_in(key, 12)
    key_cols = jax.random.fold_in(key, 13)
    rows = jnp.exp(jax.random.uniform(key_rows, (TOKENS, 1), jnp.float32, 0.0, math.log(10.0)))
    cols = jnp.exp(jax.random.uniform(key_cols, (1, D), jnp.float32, 0.0, math.log(10.0)))
    base_output = jax.random.normal(key_base, (TOKENS, D), jnp.float32)
    return (base_output * rows * cols).astype(jnp.bfloat16)


def draw_adapter_table(key, part):
    key_base = jax.random.fold_in(key, 21)
    shape = (N_MP, N_ACTOR, BLK, 2 * R)
    base_output = jax.random.normal(key_base, shape, jnp.float32)
    scales = jnp.concatenate([jnp.full((R,), D ** (-0.5), jnp.float32), jnp.full((R,), R ** (-0.5), jnp.float32)])
    return base_output * scales


def place_ends(array, rng, least, high):
    longest = array.shape.index(max(array.shape))
    spots = []
    for shift in (0, 1):
        where = [jax.random.randint(jax.random.fold_in(rng, axis), (), 0, length) for axis, length in enumerate(array.shape)]
        where[longest] = (where[longest] + shift) % array.shape[longest]
        spots.append(tuple(where))
    return array.at[spots[0]].set(least).at[spots[1]].set(high)


def with_spikes(values, own_key, source, target, shards_of, factor):
    owner, partner = [(jnp.arange(values.shape[dim]) // (values.shape[dim] // shards_of)).reshape([-1 if axis == dim else 1 for axis in range(values.ndim)]) for dim in (source, target)]
    chosen = jax.random.permutation(own_key, shards_of)[partner]
    strong = (owner == chosen) | (owner == (partner + shards_of // 2) % shards_of)
    return jnp.where(strong, factor * values, values)


def block_scale(key, extent, cuts, low, high):
    def one(axis_at, parts):
        steps = jax.random.uniform(jax.random.fold_in(jax.random.fold_in(key, 6), axis_at), (parts,), jnp.float32, low / len(cuts), high / len(cuts))
        return jnp.repeat(jnp.exp(steps), extent[axis_at] // parts).reshape((-1,) + (1,) * (len(extent) - axis_at - 1))

    gain = one(*cuts[0])
    for cut in cuts[1:]:
        gain = gain * one(*cut)
    return gain


def noise(own_key, extent, deviation, reach, shards=(), held_as=jnp.bfloat16):
    factor_of = block_scale(own_key, extent, shards, -0.22, 0.18) if shards else 1.0
    array = jax.random.normal(own_key, extent, jnp.float32) * deviation * factor_of
    return jnp.minimum(jnp.maximum(array, -reach), reach).astype(held_as)


def gaussian_with(stream_key, extent, spread, limit, cuts, heavy, held_as=jnp.bfloat16):
    drawn = spread * jax.random.normal(stream_key, extent, jnp.float32)
    if cuts:
        drawn = drawn * block_scale(stream_key, extent, cuts, -0.22, 0.18)
    return jnp.clip(with_spikes(drawn, jax.random.fold_in(stream_key, 3), *heavy), -limit, limit).astype(held_as)


def setup_inputs(seed: int = 0) -> dict:
    key_list = jax.random.split(jax.random.key(seed), 10)
    return {
        "resid": draw_resid(jax.random.fold_in(key_list[9], 71), 0),
        "norm_gain": jnp.clip(1.0 + 0.15 * jax.random.normal(key_list[1], (D,), jnp.float32), 0.25, 1.75).astype(jnp.bfloat16),
        "query_weight": noise(key_list[2], (D, D), D ** -0.5, 0.09375, ((1, 8),)),
        "cotangent": gaussian_with(key_list[3], (TOKENS, D), 0.1, 1.25, ((0, 32), (1, 8)), (0, 1, 32, 2.75)),
        "lengths": place_ends(jax.random.randint(key_list[4], (NSEQ,), 1, LEN + 1), jax.random.fold_in(key_list[4], 1), 1, LEN).astype(jnp.int32),
        "owner": jax.random.permutation(key_list[5], N_ACTOR).astype(jnp.int32),
        "adapter_table": draw_adapter_table(jax.random.fold_in(key_list[9], 71), 0),
        "moment_one": noise(key_list[7], (N_MP, N_ACTOR, BLK, 2 * R), 0.5, 3.0, ((0, 8), (1, 32)), jnp.float32),
        "moment_two": jnp.clip(jnp.exp(math.log(0.1) - 3.506558 * jax.random.uniform(key_list[8], (N_MP, N_ACTOR, BLK, 2 * R), jnp.float32) ** block_scale(key_list[8], (N_MP, N_ACTOR, BLK, 2 * R), ((0, 8), (1, 32)), -0.2, 0.2)), 0.003, 0.1),
    }


adapter_scale = 0.5
learn_rate = 0.003
beta_one = 0.9
beta_two = 0.999
fix_one = 1.0 - 0.9 ** 10
fix_two = 1.0 - 0.999 ** 10

def build_table(owned, owner):
    ordered = jnp.take(owned, owner, axis=1)
    return ordered.reshape(D, 2 * R)

def reference(resid, norm_gain, query_weight, cotangent, lengths, owner, adapter_table, moment_one, moment_two):
    stream = resid.astype(jnp.float32)
    meansq = lax.optimization_barrier(jnp.mean(stream * stream, axis=1, keepdims=True))
    normalized_input = (stream * lax.rsqrt(meansq + 1e-05) * norm_gain.astype(jnp.float32)[None, :]).astype(jnp.bfloat16)
    index = jnp.arange(TOKENS, dtype=jnp.int32)
    position = index % LEN
    sequence = index // LEN
    active_rows = position < jnp.take(lengths, sequence)
    adapter_now = build_table(adapter_table, owner).astype(jnp.bfloat16)
    mat_a = adapter_now[:, :R]
    mat_bt = adapter_now[:, R:]
    lowrank_output = jnp.dot(normalized_input, mat_a, preferred_element_type=jnp.float32).astype(jnp.bfloat16)
    base_output = jnp.dot(normalized_input, query_weight, preferred_element_type=jnp.float32)
    extra_term = jnp.dot(lowrank_output, mat_bt.T, preferred_element_type=jnp.float32)
    query = jnp.where(active_rows[:, None], base_output + adapter_scale * extra_term, 0.0).astype(jnp.bfloat16)
    masked_rows = jnp.where(active_rows[:, None], cotangent, jnp.zeros_like(cotangent))
    backward_rows = jnp.dot(masked_rows, mat_bt, preferred_element_type=jnp.float32).astype(jnp.bfloat16)
    down_gradient = adapter_scale * jnp.dot(normalized_input.T, backward_rows, preferred_element_type=jnp.float32)
    up_transposed_gradient = adapter_scale * jnp.dot(masked_rows.T, lowrank_output, preferred_element_type=jnp.float32)
    grad = jnp.concatenate([down_gradient, up_transposed_gradient], axis=1)
    grad_blocks = grad.reshape(N_MP, N_ACTOR, BLK, 2 * R)
    grad_owned = jnp.zeros_like(grad_blocks).at[:, owner].set(grad_blocks)
    moment_one_new = beta_one * moment_one + (1.0 - beta_one) * grad_owned
    moment_two_new = beta_two * moment_two + (1.0 - beta_two) * grad_owned * grad_owned
    adapter_new = adapter_table - learn_rate * (moment_one_new / fix_one) / (jnp.sqrt(moment_two_new / fix_two) + 1e-08)
    fresh = build_table(adapter_new, owner).astype(jnp.bfloat16)
    matmul_product = jnp.dot(fresh[:, :R], fresh[:, R:].T, preferred_element_type=jnp.float32)
    merged = (query_weight.astype(jnp.float32) + adapter_scale * matmul_product).astype(jnp.bfloat16)
    return (query, adapter_new, moment_one_new, moment_two_new, merged)
```

```python
import jax
import jax.numpy as jnp
from jax import lax
from jax.sharding import PartitionSpec as P

LEN = 256


adapter_scale = 0.5
learn_rate = 0.003
beta_one = 0.9
beta_two = 0.999
fix_one = 1.0 - 0.9**10
fix_two = 1.0 - 0.999**10


def core_swap(x):
    size = lax.axis_size("mp")
    return lax.ppermute(x, "mp", [(i, i ^ 1) for i in range(size)])


def chip_shift(x, hops):
    size = lax.axis_size("mp")
    return lax.ppermute(x, "mp", [(i, (i + 2 * hops) % size) for i in range(size)])


def summed_over_mp(partial, core):
    tokens, n = partial.shape
    half = tokens // 2
    chips = lax.axis_size("mp") // 2
    keep = lax.dynamic_slice_in_dim(partial, core * half, half, 0)
    give = lax.dynamic_slice_in_dim(partial, (1 - core) * half, half, 0)
    own = keep + core_swap(give)
    sent = own.astype(jnp.bfloat16)
    hops = sorted(range(1, chips), key=lambda k: -min(k, chips - k))
    total = own
    for k in hops:
        total = total + chip_shift(sent, k).astype(jnp.float32)
    mine = total.astype(jnp.bfloat16)
    other = core_swap(mine)
    low = jnp.where(core == 0, mine, other)
    high = jnp.where(core == 0, other, mine)
    return jnp.concatenate([low, high], axis=0)


def dot_rows(left, right):
    return lax.dot_general(
        left, right, (((0,), (0,)), ((), ())), preferred_element_type=jnp.float32
    )


def dot_columns(left, right):
    return lax.dot_general(
        left, right, (((1,), (1,)), ((), ())), preferred_element_type=jnp.float32
    )


def body(
    resid, norm_gain, query_weight, cotangent, lengths, owner, adapter_table, moment_one, moment_two
):
    n_actor = lax.axis_size("actor")
    n_mp = lax.axis_size("mp")
    mp_index = lax.axis_index("mp")
    actor_index = lax.axis_index("actor")
    core = mp_index % 2
    tokens, width = resid.shape
    cols = query_weight.shape[1]
    block = adapter_table.shape[2]
    rank = adapter_table.shape[3] // 2
    now = adapter_table.reshape(block, 2 * rank).astype(jnp.bfloat16)
    part = lax.all_to_all(
        jnp.broadcast_to(now[None], (n_actor, block, 2 * rank)), "actor", 0, 0, tiled=True
    )
    mine = jnp.take(part, owner, axis=0).reshape(cols, 2 * rank)
    stream = resid.astype(jnp.float32)
    meansq = jnp.mean(stream * stream, axis=1, keepdims=True)
    normed = (
        stream * lax.rsqrt(meansq + 1e-05) * norm_gain.astype(jnp.float32)[None, :]
    ).astype(jnp.bfloat16)
    index = jnp.arange(tokens, dtype=jnp.int32)
    seq_ids = jnp.arange(lengths.shape[0], dtype=jnp.int32)
    live = jnp.any(
        ((index // LEN)[:, None] == seq_ids[None, :])
        & ((index % LEN)[:, None] < lengths[None, :]),
        axis=1,
    )
    masked = jnp.where(live[:, None], cotangent, jnp.zeros_like(cotangent))
    normed_local = lax.dynamic_slice_in_dim(normed, mp_index * cols, cols, 1)
    low_part = jnp.dot(normed_local, mine[:, :rank], preferred_element_type=jnp.float32)
    back_part = jnp.dot(masked, mine[:, rank:], preferred_element_type=jnp.float32)
    both = summed_over_mp(jnp.concatenate([low_part, back_part], axis=1), core)
    low = both[:, :rank]
    back = both[:, rank:]
    base = jnp.dot(normed, query_weight, preferred_element_type=jnp.float32)
    extra = dot_columns(low, mine[:, rank:])
    query = jnp.where(live[:, None], base + adapter_scale * extra, 0.0).astype(jnp.bfloat16)
    grad = adapter_scale * jnp.concatenate(
        [dot_rows(normed_local, back), dot_rows(masked, low)], axis=1
    )
    actors = jnp.arange(n_actor, dtype=jnp.int32)
    inverse = jnp.sum(jnp.where(owner[None, :] == actors[:, None], actors[None, :], 0), axis=1)
    sent = jnp.take(grad.reshape(n_actor, block, 2 * rank), inverse, axis=0)
    summed = lax.all_to_all(sent, "actor", 0, 0, tiled=True).sum(axis=0)
    first = beta_one * moment_one.reshape(block, 2 * rank) + (1.0 - beta_one) * summed
    second = beta_two * moment_two.reshape(block, 2 * rank) + (1.0 - beta_two) * summed * summed
    updated = adapter_table.reshape(block, 2 * rank) - learn_rate * (first / fix_one) / (
        jnp.sqrt(second / fix_two) + 1e-08
    )
    fresh = updated.astype(jnp.bfloat16)
    slices = lax.all_gather(fresh, "mp")
    ratio = n_actor // n_mp
    a_out = jnp.broadcast_to(
        slices[:, None, :, :rank], (n_mp, ratio, block, rank)
    ).reshape(n_actor, block, rank)
    b_out = jnp.broadcast_to(fresh[None, :, rank:], (n_actor, block, rank))
    got = lax.all_to_all(jnp.concatenate([a_out, b_out], axis=2), "actor", 0, 0, tiled=True)
    ordered = jnp.take(got, owner, axis=0).reshape(cols, 2 * rank)
    row_count = width // n_actor
    a_rows = lax.dynamic_slice_in_dim(ordered, actor_index % ratio * row_count, row_count, 0)
    weight_rows = lax.dynamic_slice_in_dim(query_weight, actor_index * row_count, row_count, 0)
    merged = (
        weight_rows.astype(jnp.float32)
        + adapter_scale * dot_columns(a_rows[:, :rank], ordered[:, rank:])
    ).astype(jnp.bfloat16)
    shape = adapter_table.shape
    return (query, updated.reshape(shape), first.reshape(shape), second.reshape(shape), merged)


def solution(mesh):
    return jax.shard_map(
        body,
        mesh=mesh,
        in_specs=(
            P("actor", None),
            P(),
            P(None, "mp"),
            P("actor", "mp"),
            P("actor"),
            P(),
            P("mp", "actor", None, None),
            P("mp", "actor", None, None),
            P("mp", "actor", None, None),
        ),
        out_specs=(
            P("actor", "mp"),
            P("mp", "actor", None, None),
            P("mp", "actor", None, None),
            P("mp", "actor", None, None),
            P("actor", "mp"),
        ),
        check_vma=False,
    )
```

```python
import jax
import jax.numpy as jnp
from jax import lax
from jax.experimental import pallas as pl
from jax.experimental.pallas import tpu as pltpu
from jax.sharding import PartitionSpec as P

LEN = 256


adapter_scale = 0.5
learn_rate = 0.003
beta_one = 0.9
beta_two = 0.999
fix_one = 1.0 - 0.9**10
fix_two = 1.0 - 0.999**10

f32 = jnp.float32
bf16 = jnp.bfloat16


def lanes_of(shape):
    return lax.broadcasted_iota(jnp.int32, shape, 1)


def dot_nt(left, right):
    return lax.dot_general(left, right, (((1,), (1,)), ((), ())), preferred_element_type=f32)


def norm_kernel(place_ref, x_ref, g_ref, w_ref, base_ref, local_ref, own_ref, n_ref):
    rows, width = x_ref.shape
    cols = base_ref.shape[1]
    own_rows = own_ref.shape[0]
    own_ref[...] = w_ref[pl.ds(pl.multiple_of(place_ref[2] * own_rows, own_rows), own_rows), :]
    for r in range(0, rows, 16):
        acc = jnp.zeros((16, 128), f32)
        for c in range(0, width, 128):
            x = x_ref[r : r + 16, c : c + 128].astype(f32)
            acc = acc + x * x
        mean = jnp.sum(acc, axis=1, keepdims=True) * (1.0 / width)
        scale = jnp.broadcast_to(lax.rsqrt(mean + 1e-05), (16, 128))
        for c in range(0, width, 128):
            x = x_ref[r : r + 16, c : c + 128].astype(f32)
            n_ref[r : r + 16, c : c + 128] = (x * scale * g_ref[:, c : c + 128]).astype(bf16)
    start = pl.multiple_of(place_ref[0] * cols, cols)
    local_ref[...] = n_ref[:, pl.ds(start, cols)]
    base_ref[...] = jnp.dot(n_ref[...], w_ref[...], preferred_element_type=f32)


def norm_and_project(place, resid, gain, weight, own_rows, rows=256):
    tokens, width = resid.shape
    cols = weight.shape[1]
    gains = jnp.broadcast_to(gain.astype(f32)[None], (16, width))
    return pl.pallas_call(
        norm_kernel,
        grid_spec=pltpu.PrefetchScalarGridSpec(
            num_scalar_prefetch=1,
            grid=(tokens // rows,),
            in_specs=[
                pl.BlockSpec((rows, width), lambda i, s: (i, 0)),
                pl.BlockSpec((16, width), lambda i, s: (0, 0)),
                pl.BlockSpec((width, cols), lambda i, s: (0, 0)),
            ],
            out_specs=[
                pl.BlockSpec((rows, cols), lambda i, s: (i, 0)),
                pl.BlockSpec((rows, cols), lambda i, s: (i, 0)),
                pl.BlockSpec((own_rows, cols), lambda i, s: (0, 0)),
            ],
            scratch_shapes=[pltpu.VMEM((rows, width), bf16)],
        ),
        out_shape=[
            jax.ShapeDtypeStruct((tokens, cols), f32),
            jax.ShapeDtypeStruct((tokens, cols), bf16),
            jax.ShapeDtypeStruct((own_rows, cols), bf16),
        ],
        compiler_params=pltpu.CompilerParams(vmem_limit_bytes=58 * 2**20),
        cost_estimate=pl.CostEstimate(
            flops=2 * tokens * width * cols,
            bytes_accessed=2 * tokens * width + 2 * width * cols + 6 * tokens * cols,
            transcendentals=0,
        ),
        name="norm_and_project",
    )(place, resid, gains, weight)


def live_rows(lengths_ref, sequence, shape):
    return lax.broadcasted_iota(jnp.int32, shape, 0) < lengths_ref[sequence]


def parts_kernel(
    place_ref, owner_ref, lengths_ref, got_ref, local_ref, cot_ref,
    table_ref, keep_ref, give_ref, part_ref,
):
    blocks, block, lanes = got_ref.shape
    for j in range(blocks):
        table_ref[j * block : (j + 1) * block, :] = got_ref[owner_ref[j]]
    swapped = pltpu.roll(table_ref[...].astype(f32), lanes // 2, 1).astype(bf16)
    tokens = local_ref.shape[0]
    for s in range(tokens // LEN):
        rows = slice(s * LEN, (s + 1) * LEN)
        back = jnp.dot(cot_ref[rows, :], swapped, preferred_element_type=f32)
        low = jnp.dot(local_ref[rows, :], swapped, preferred_element_type=f32)
        both = jnp.where(lanes_of(back.shape) < lanes // 2, back, low)
        part_ref[rows, :] = jnp.where(live_rows(lengths_ref, s, both.shape), both, 0.0)
    half = tokens // 2
    core = place_ref[1]
    keep_ref[...] = part_ref[pl.ds(pl.multiple_of(core * half, half), half), :]
    give_ref[...] = part_ref[pl.ds(pl.multiple_of((1 - core) * half, half), half), :]


def whole(n_scalar, n_in, n_out, scratch=()):
    return pltpu.PrefetchScalarGridSpec(
        num_scalar_prefetch=n_scalar,
        grid=(),
        in_specs=[pl.BlockSpec(memory_space=pltpu.VMEM)] * n_in,
        out_specs=[pl.BlockSpec(memory_space=pltpu.VMEM)] * n_out,
        scratch_shapes=list(scratch),
    )


small = pltpu.CompilerParams(vmem_limit_bytes=16 * 2**20)


def cost(flops, moved):
    return pl.CostEstimate(flops=flops, bytes_accessed=moved, transcendentals=0)


def partial_products(place, owner, lengths, got, local, cot):
    blocks, block, lanes = got.shape
    tokens, cols = local.shape
    half = jax.ShapeDtypeStruct((tokens // 2, lanes), f32)
    return pl.pallas_call(
        parts_kernel,
        grid_spec=whole(3, 3, 3, [pltpu.VMEM((tokens, lanes), f32)]),
        out_shape=[jax.ShapeDtypeStruct((cols, lanes), bf16), half, half],
        compiler_params=small,
        cost_estimate=cost(4 * tokens * cols * lanes, 4 * tokens * cols + 4 * tokens * lanes),
        name="partial_products",
    )(place, owner, lengths, got, local, cot)


def grads_kernel(place_ref, owner_ref, mine_ref, other_ref, local_ref, cot_ref, both_ref, sent_ref, g_ref):
    half, lanes = mine_ref.shape
    core = place_ref[1]
    both_ref[pl.ds(pl.multiple_of(core * half, half), half), :] = mine_ref[...]
    both_ref[pl.ds(pl.multiple_of((1 - core) * half, half), half), :] = other_ref[...]
    turned = both_ref[...].T
    rank = lanes // 2
    down = jnp.dot(turned[:rank], local_ref[...], preferred_element_type=f32)
    up = jnp.dot(turned[rank:], cot_ref[...], preferred_element_type=f32)
    g_ref[...] = adapter_scale * jnp.concatenate([down, up], axis=0).T
    blocks, block, _ = sent_ref.shape
    for j in range(blocks):
        sent_ref[owner_ref[j]] = g_ref[j * block : (j + 1) * block, :].astype(bf16)


def gradients(place, owner, mine, other, local, cot):
    half, lanes = mine.shape
    tokens, cols = local.shape
    blocks = owner.shape[0]
    return pl.pallas_call(
        grads_kernel,
        grid_spec=whole(2, 4, 2, [pltpu.VMEM((cols, lanes), f32)]),
        out_shape=[
            jax.ShapeDtypeStruct((tokens, lanes), bf16),
            jax.ShapeDtypeStruct((blocks, cols // blocks, lanes), bf16),
        ],
        compiler_params=small,
        cost_estimate=cost(2 * tokens * cols * lanes, 4 * tokens * cols + 4 * cols * lanes),
        name="gradients",
    )(place, owner, mine, other, local, cot)


def query_kernel(lengths_ref, base_ref, both_ref, table_ref, out_ref):
    lanes = both_ref.shape[1]
    table = table_ref[...].astype(f32)
    up = jnp.where(lanes_of(table.shape) >= lanes // 2, table, 0.0).astype(bf16)
    value = base_ref[...] + adapter_scale * dot_nt(both_ref[...], up)
    live = live_rows(lengths_ref, pl.program_id(0), value.shape)
    out_ref[...] = jnp.where(live, value, 0.0).astype(bf16)


def finished_query(lengths, base, both, table):
    tokens, cols = base.shape
    lanes = both.shape[1]
    return pl.pallas_call(
        query_kernel,
        grid_spec=pltpu.PrefetchScalarGridSpec(
            num_scalar_prefetch=1,
            grid=(tokens // LEN,),
            in_specs=[
                pl.BlockSpec((LEN, cols), lambda i, s: (i, 0)),
                pl.BlockSpec((LEN, lanes), lambda i, s: (i, 0)),
                pl.BlockSpec((cols, lanes), lambda i, s: (0, 0)),
            ],
            out_specs=[pl.BlockSpec((LEN, cols), lambda i, s: (i, 0))],
        ),
        out_shape=[jax.ShapeDtypeStruct((tokens, cols), bf16)],
        compiler_params=small,
        cost_estimate=cost(2 * tokens * cols * lanes, 6 * tokens * cols),
        name="finished_query",
    )(lengths, base, both, table)[0]


def offer_kernel(place_ref, *refs):
    slices, out_ref = refs[:-1], refs[-1]
    lanes = out_ref.shape[2]
    n_mp = len(slices)
    ratio = out_ref.shape[0] // n_mp
    own = slices[0][...]
    for k, ref in enumerate(slices):
        source = lax.rem(place_ref[0] - k + n_mp, n_mp)
        value = jnp.where(
            lanes_of(own.shape) < lanes // 2, ref[...].astype(f32), own.astype(f32)
        ).astype(bf16)
        for q in range(ratio):
            out_ref[source * ratio + q] = value


def offered(place, slices, n_actor):
    block, lanes = slices[0].shape
    return pl.pallas_call(
        offer_kernel,
        grid_spec=pltpu.PrefetchScalarGridSpec(
            num_scalar_prefetch=1,
            grid=(),
            in_specs=[pl.BlockSpec(memory_space=pltpu.VMEM)] * len(slices),
            out_specs=[pl.BlockSpec(memory_space=pltpu.VMEM)],
        ),
        out_shape=[jax.ShapeDtypeStruct((n_actor, block, lanes), bf16)],
        compiler_params=small,
        name="offered",
    )(place, *slices)[0]


def merge_kernel(place_ref, owner_ref, got_ref, w_ref, out_ref, t_ref):
    blocks, block, lanes = got_ref.shape
    for j in range(blocks):
        t_ref[j * block : (j + 1) * block, :] = got_ref[owner_ref[j]]
    rows = out_ref.shape[0]
    start = pl.multiple_of(place_ref[3] * rows, rows)
    down = pltpu.roll(t_ref[pl.ds(start, rows), :].astype(f32), lanes // 2, 1).astype(bf16)
    table = t_ref[...].astype(f32)
    up = jnp.where(lanes_of(table.shape) >= lanes // 2, table, 0.0).astype(bf16)
    out_ref[...] = (w_ref[...].astype(f32) + adapter_scale * dot_nt(down, up)).astype(bf16)


def merge(place, owner, got, weight_rows):
    blocks, block, lanes = got.shape
    return pl.pallas_call(
        merge_kernel,
        grid_spec=whole(2, 2, 1, [pltpu.VMEM((blocks * block, lanes), bf16)]),
        out_shape=[jax.ShapeDtypeStruct(weight_rows.shape, bf16)],
        compiler_params=small,
        name="merge",
    )(place, owner, got, weight_rows)[0]


def core_swap(x):
    size = lax.axis_size("mp")
    return lax.ppermute(x, "mp", [(i, i ^ 1) for i in range(size)])


def mp_shift(x, k):
    size = lax.axis_size("mp")
    return lax.ppermute(x, "mp", [(i, (i + k) % size) for i in range(size)])


def farthest_first(n):
    return sorted(range(1, n), key=lambda k: -min(k, n - k))


def body(
    resid, norm_gain, query_weight, cotangent, lengths, owner, adapter_table, moment_one, moment_two
):
    n_actor = lax.axis_size("actor")
    n_mp = lax.axis_size("mp")
    mp_index = lax.axis_index("mp")
    actor_index = lax.axis_index("actor")
    ratio = n_actor // n_mp
    place = jnp.stack([mp_index, mp_index % 2, actor_index, actor_index % ratio]).astype(jnp.int32)
    block = adapter_table.shape[2]
    lanes = adapter_table.shape[3]
    rank = lanes // 2
    table_now = adapter_table.reshape(block, lanes)
    got = lax.all_to_all(
        jnp.broadcast_to(table_now.astype(bf16)[None], (n_actor, block, lanes)),
        "actor", 0, 0, tiled=True,
    )
    base, local, weight_rows = norm_and_project(
        place, resid, norm_gain, query_weight, resid.shape[1] // n_actor
    )
    table, keep, give = partial_products(place, owner, lengths, got, local, cotangent)
    own = keep + core_swap(give)
    sent = own.astype(bf16)
    total = own
    for k in farthest_first(n_mp // 2):
        total = total + mp_shift(sent, 2 * k).astype(f32)
    mine = total.astype(bf16)
    both, grad = gradients(place, owner, mine, core_swap(mine), local, cotangent)
    received = lax.all_to_all(grad, "actor", 0, 0, tiled=True)
    summed = received.astype(f32).sum(axis=0)
    first = beta_one * moment_one.reshape(block, lanes) + (1.0 - beta_one) * summed
    second = beta_two * moment_two.reshape(block, lanes) + (1.0 - beta_two) * summed * summed
    updated = table_now - learn_rate * (first / fix_one) / (jnp.sqrt(second / fix_two) + 1e-08)
    fresh = updated.astype(bf16)
    slices = [fresh] + [None] * (n_mp - 1)
    for k in farthest_first(n_mp):
        slices[k] = mp_shift(fresh, k)
    query = finished_query(lengths, base, both, table)
    fresh_got = lax.all_to_all(offered(place, slices, n_actor), "actor", 0, 0, tiled=True)
    merged = merge(place, owner, fresh_got, weight_rows)
    shape = adapter_table.shape
    return (query, updated.reshape(shape), first.reshape(shape), second.reshape(shape), merged)


def solution(mesh):
    return jax.shard_map(
        body,
        mesh=mesh,
        in_specs=(
            P("actor", None),
            P(),
            P(None, "mp"),
            P("actor", "mp"),
            P("actor"),
            P(),
            P("mp", "actor", None, None),
            P("mp", "actor", None, None),
            P("mp", "actor", None, None),
        ),
        out_specs=(
            P("actor", "mp"),
            P("mp", "actor", None, None),
            P("mp", "actor", None, None),
            P("mp", "actor", None, None),
            P("actor", "mp"),
        ),
        check_vma=False,
    )
```

```python
import jax
import jax.numpy as jnp
from jax import lax
from jax.experimental import pallas as pl
from jax.experimental.pallas import tpu as pltpu
from jax.sharding import PartitionSpec as P

LEN = 256


adapter_scale = 0.5
learn_rate = 0.003
beta_one = 0.9
beta_two = 0.999
fix_one = 1.0 - 0.9**10
fix_two = 1.0 - 0.999**10

f32 = jnp.float32
bf16 = jnp.bfloat16


def lanes_of(shape):
    return lax.broadcasted_iota(jnp.int32, shape, 1)


def dot_nt(left, right):
    return lax.dot_general(left, right, (((1,), (1,)), ((), ())), preferred_element_type=f32)


def norm_kernel(x_ref, g_ref, w_ref, base_ref, local_ref, own_ref, n_ref):
    rows, width = x_ref.shape
    cols = base_ref.shape[1]
    own_rows = own_ref.shape[0]
    first = pl.multiple_of(lax.axis_index("actor") * own_rows, own_rows)
    own_ref[...] = w_ref[pl.ds(first, own_rows), :]
    for r in range(0, rows, 16):
        acc = jnp.zeros((16, 128), f32)
        for c in range(0, width, 128):
            x = x_ref[r : r + 16, c : c + 128].astype(f32)
            acc = acc + x * x
        mean = jnp.sum(acc, axis=1, keepdims=True) * (1.0 / width)
        scale = jnp.broadcast_to(lax.rsqrt(mean + 1e-05), (16, 128))
        for c in range(0, width, 128):
            x = x_ref[r : r + 16, c : c + 128].astype(f32)
            n_ref[r : r + 16, c : c + 128] = (x * scale * g_ref[:, c : c + 128]).astype(bf16)
    start = pl.multiple_of(lax.axis_index("mp") * cols, cols)
    local_ref[...] = n_ref[:, pl.ds(start, cols)]
    base_ref[...] = jnp.dot(n_ref[...], w_ref[...], preferred_element_type=f32)


def norm_and_project(resid, gains, weight, own_rows, rows=512):
    tokens, width = resid.shape
    cols = weight.shape[1]
    return pl.pallas_call(
        norm_kernel,
        grid_spec=pltpu.PrefetchScalarGridSpec(
            num_scalar_prefetch=0,
            grid=(tokens // rows,),
            in_specs=[
                pl.BlockSpec((rows, width), lambda i: (i, 0)),
                pl.BlockSpec((16, width), lambda i: (0, 0)),
                pl.BlockSpec((width, cols), lambda i: (0, 0)),
            ],
            out_specs=[
                pl.BlockSpec((rows, cols), lambda i: (i, 0)),
                pl.BlockSpec((rows, cols), lambda i: (i, 0)),
                pl.BlockSpec((own_rows, cols), lambda i: (0, 0)),
            ],
            scratch_shapes=[pltpu.VMEM((rows, width), bf16)],
        ),
        out_shape=[
            jax.ShapeDtypeStruct((tokens, cols), f32),
            jax.ShapeDtypeStruct((tokens, cols), bf16),
            jax.ShapeDtypeStruct((own_rows, cols), bf16),
        ],
        compiler_params=pltpu.CompilerParams(vmem_limit_bytes=52 * 2**20),
        cost_estimate=pl.CostEstimate(
            flops=2 * tokens * width * cols,
            bytes_accessed=2 * tokens * width + 2 * width * cols + 6 * tokens * cols,
            transcendentals=0,
        ),
        name="norm_and_project",
    )(resid, gains, weight)


def live_rows(lengths_ref, sequence, shape):
    return lax.broadcasted_iota(jnp.int32, shape, 0) < lengths_ref[sequence]


def parts_kernel(
    owner_ref, lengths_ref, got_ref, local_ref, cot_ref,
    table_ref, keep_ref, give_ref, part_ref,
):
    blocks, block, lanes = got_ref.shape
    for j in range(blocks):
        table_ref[j * block : (j + 1) * block, :] = got_ref[owner_ref[j]]
    swapped = pltpu.roll(table_ref[...].astype(f32), lanes // 2, 1).astype(bf16)
    tokens = local_ref.shape[0]
    for s in range(tokens // LEN):
        rows = slice(s * LEN, (s + 1) * LEN)
        back = jnp.dot(cot_ref[rows, :], swapped, preferred_element_type=f32)
        low = jnp.dot(local_ref[rows, :], swapped, preferred_element_type=f32)
        both = jnp.where(lanes_of(back.shape) < lanes // 2, back, low)
        part_ref[rows, :] = jnp.where(live_rows(lengths_ref, s, both.shape), both, 0.0)
    half = tokens // 2
    core = lax.axis_index("mp") % 2
    keep_ref[...] = part_ref[pl.ds(pl.multiple_of(core * half, half), half), :]
    give_ref[...] = part_ref[pl.ds(pl.multiple_of((1 - core) * half, half), half), :]


def whole(n_scalar, n_in, n_out, scratch=()):
    return pltpu.PrefetchScalarGridSpec(
        num_scalar_prefetch=n_scalar,
        grid=(),
        in_specs=[pl.BlockSpec(memory_space=pltpu.VMEM)] * n_in,
        out_specs=[pl.BlockSpec(memory_space=pltpu.VMEM)] * n_out,
        scratch_shapes=list(scratch),
    )


small = pltpu.CompilerParams(vmem_limit_bytes=16 * 2**20)


def cost(flops, moved):
    return pl.CostEstimate(flops=flops, bytes_accessed=moved, transcendentals=0)


def partial_products(owner, lengths, got, local, cot):
    blocks, block, lanes = got.shape
    tokens, cols = local.shape
    half = jax.ShapeDtypeStruct((tokens // 2, lanes), f32)
    return pl.pallas_call(
        parts_kernel,
        grid_spec=whole(2, 3, 3, [pltpu.VMEM((tokens, lanes), f32)]),
        out_shape=[jax.ShapeDtypeStruct((cols, lanes), bf16), half, half],
        compiler_params=small,
        cost_estimate=cost(4 * tokens * cols * lanes, 4 * tokens * cols + 4 * tokens * lanes),
        name="partial_products",
    )(owner, lengths, got, local, cot)


def grads_kernel(
    owner_ref, mine_ref, other_ref, local_ref, cot_ref, both_ref, sent_ref, g_ref
):
    half, lanes = mine_ref.shape
    core = lax.axis_index("mp") % 2
    both_ref[pl.ds(pl.multiple_of(core * half, half), half), :] = mine_ref[...]
    both_ref[pl.ds(pl.multiple_of((1 - core) * half, half), half), :] = other_ref[...]
    turned = both_ref[...].T
    rank = lanes // 2
    down = jnp.dot(turned[:rank], local_ref[...], preferred_element_type=f32)
    up = jnp.dot(turned[rank:], cot_ref[...], preferred_element_type=f32)
    g_ref[...] = adapter_scale * jnp.concatenate([down, up], axis=0).T
    blocks, block, _ = sent_ref.shape
    for j in range(blocks):
        sent_ref[owner_ref[j]] = g_ref[j * block : (j + 1) * block, :].astype(bf16)


def gradients(owner, mine, other, local, cot):
    half, lanes = mine.shape
    tokens, cols = local.shape
    blocks = owner.shape[0]
    return pl.pallas_call(
        grads_kernel,
        grid_spec=whole(1, 4, 2, [pltpu.VMEM((cols, lanes), f32)]),
        out_shape=[
            jax.ShapeDtypeStruct((tokens, lanes), bf16),
            jax.ShapeDtypeStruct((blocks, cols // blocks, lanes), bf16),
        ],
        compiler_params=small,
        cost_estimate=cost(2 * tokens * cols * lanes, 4 * tokens * cols + 4 * cols * lanes),
        name="gradients",
    )(owner, mine, other, local, cot)


def query_kernel(lengths_ref, base_ref, both_ref, table_ref, out_ref, done_ref):
    lanes = both_ref.shape[1]
    table = table_ref[...].astype(f32)
    up = jnp.where(lanes_of(table.shape) >= lanes // 2, table, 0.0).astype(bf16)
    value = base_ref[...] + adapter_scale * dot_nt(both_ref[...], up)
    live = live_rows(lengths_ref, pl.program_id(0), value.shape)
    out_ref[...] = jnp.where(live, value, 0.0).astype(bf16)
    done_ref[...] = jnp.zeros_like(done_ref)


def finished_query(lengths, base, both, table):
    tokens, cols = base.shape
    lanes = both.shape[1]
    return pl.pallas_call(
        query_kernel,
        grid_spec=pltpu.PrefetchScalarGridSpec(
            num_scalar_prefetch=1,
            grid=(tokens // LEN,),
            in_specs=[
                pl.BlockSpec((LEN, cols), lambda i, s: (i, 0)),
                pl.BlockSpec((LEN, lanes), lambda i, s: (i, 0)),
                pl.BlockSpec((cols, lanes), lambda i, s: (0, 0)),
            ],
            out_specs=[
                pl.BlockSpec((LEN, cols), lambda i, s: (i, 0)),
                pl.BlockSpec((16, 128), lambda i, s: (0, 0)),
            ],
        ),
        out_shape=[
            jax.ShapeDtypeStruct((tokens, cols), bf16),
            jax.ShapeDtypeStruct((16, 128), f32),
        ],
        compiler_params=small,
        cost_estimate=cost(2 * tokens * cols * lanes, 6 * tokens * cols),
        name="finished_query",
    )(lengths, base, both, table)


def offer_kernel(slices_ref, own_ref, out_ref):
    n_mp, block, lanes = slices_ref.shape
    ratio = out_ref.shape[0] // n_mp
    own = own_ref[...].astype(f32)
    for m in range(n_mp):
        down = slices_ref[m].astype(f32)
        value = jnp.where(lanes_of(own.shape) < lanes // 2, down, own).astype(bf16)
        for q in range(ratio):
            out_ref[m * ratio + q] = value


def offered(slices, own, n_actor):
    block, lanes = own.shape
    return pl.pallas_call(
        offer_kernel,
        grid_spec=whole(0, 2, 1),
        out_shape=[jax.ShapeDtypeStruct((n_actor, block, lanes), bf16)],
        compiler_params=small,
        name="offered",
    )(slices, own)[0]


def merge_kernel(owner_ref, got_ref, w_ref, out_ref, t_ref):
    blocks, block, lanes = got_ref.shape
    for j in range(blocks):
        t_ref[j * block : (j + 1) * block, :] = got_ref[owner_ref[j]]
    rows = out_ref.shape[0]
    start = pl.multiple_of(lax.axis_index("actor") % (t_ref.shape[0] // rows) * rows, rows)
    down = pltpu.roll(t_ref[pl.ds(start, rows), :].astype(f32), lanes // 2, 1).astype(bf16)
    table = t_ref[...].astype(f32)
    up = jnp.where(lanes_of(table.shape) >= lanes // 2, table, 0.0).astype(bf16)
    out_ref[...] = (w_ref[...].astype(f32) + adapter_scale * dot_nt(down, up)).astype(bf16)


def merge(owner, got, weight_rows):
    blocks, block, lanes = got.shape
    return pl.pallas_call(
        merge_kernel,
        grid_spec=whole(1, 2, 1, [pltpu.VMEM((blocks * block, lanes), bf16)]),
        out_shape=[jax.ShapeDtypeStruct(weight_rows.shape, bf16)],
        compiler_params=small,
        name="merge",
    )(owner, got, weight_rows)[0]


def core_swap(x):
    size = lax.axis_size("mp")
    return lax.ppermute(x, "mp", [(i, i ^ 1) for i in range(size)])


def chip_shift(x, hops):
    size = lax.axis_size("mp")
    return lax.ppermute(x, "mp", [(i, (i + 2 * hops) % size) for i in range(size)])


def exchanged(x, copies, axis):
    spread = jnp.broadcast_to(x[None], (copies, *x.shape))
    return lax.all_to_all(spread, axis, 0, 0, tiled=True)


def body(
    resid, norm_gain, query_weight, cotangent, lengths, owner, adapter_table, moment_one, moment_two
):
    n_actor = lax.axis_size("actor")
    n_mp = lax.axis_size("mp")
    chips = n_mp // 2
    block = adapter_table.shape[2]
    lanes = adapter_table.shape[3]
    table_now = adapter_table.reshape(block, lanes)
    got = exchanged(table_now.astype(bf16), n_actor, "actor")
    gains = jnp.broadcast_to(norm_gain.astype(f32)[None], (16, resid.shape[1]))
    base, local, weight_rows = norm_and_project(
        resid, gains, query_weight, resid.shape[1] // n_actor
    )
    table, keep, give = partial_products(owner, lengths, got, local, cotangent)
    own = keep + core_swap(give)
    sent = own.astype(bf16)
    total = own
    for hops in sorted(range(1, chips), key=lambda k: min(k, chips - k)):
        total = total + chip_shift(sent, hops).astype(f32)
    mine = total.astype(bf16)
    both, grad = gradients(owner, mine, core_swap(mine), local, cotangent)
    received = lax.all_to_all(grad, "actor", 0, 0, tiled=True)
    query, done = finished_query(lengths, base, both, table)
    summed = received.astype(f32).sum(axis=0) + done
    first = beta_one * moment_one.reshape(block, lanes) + (1.0 - beta_one) * summed
    second = beta_two * moment_two.reshape(block, lanes) + (1.0 - beta_two) * summed * summed
    updated = table_now - learn_rate * (first / fix_one) / (jnp.sqrt(second / fix_two) + 1e-08)
    fresh = updated.astype(bf16)
    slices = exchanged(fresh, n_mp, "mp")
    fresh_got = lax.all_to_all(offered(slices, fresh, n_actor), "actor", 0, 0, tiled=True)
    merged = merge(owner, fresh_got, weight_rows)
    shape = adapter_table.shape
    return (query, updated.reshape(shape), first.reshape(shape), second.reshape(shape), merged)


def solution(mesh):
    return jax.shard_map(
        body,
        mesh=mesh,
        in_specs=(
            P("actor", None),
            P(),
            P(None, "mp"),
            P("actor", "mp"),
            P("actor"),
            P(),
            P("mp", "actor", None, None),
            P("mp", "actor", None, None),
            P("mp", "actor", None, None),
        ),
        out_specs=(
            P("actor", "mp"),
            P("mp", "actor", None, None),
            P("mp", "actor", None, None),
            P("mp", "actor", None, None),
            P("actor", "mp"),
        ),
        check_vma=False,
    )
```

```python
import jax
import jax.numpy as jnp
from jax import lax
from jax.experimental import pallas as pl
from jax.experimental.pallas import tpu as pltpu
from jax.sharding import PartitionSpec as P

LEN = 256


adapter_scale = 0.5
learn_rate = 0.003
beta_one = 0.9
beta_two = 0.999
fix_one = 1.0 - 0.9**10
fix_two = 1.0 - 0.999**10

f32 = jnp.float32
bf16 = jnp.bfloat16


def lanes_of(shape):
    return lax.broadcasted_iota(jnp.int32, shape, 1)


def dot_nt(left, right):
    return lax.dot_general(left, right, (((1,), (1,)), ((), ())), preferred_element_type=f32)


def norm_kernel(x_ref, gain_ref, w_ref, base_ref, local_ref, own_ref, n_ref, g_ref):
    rows, width = x_ref.shape
    cols = base_ref.shape[1]
    g_ref[...] = jnp.broadcast_to(gain_ref[...].astype(f32)[None, :], g_ref.shape)
    own_rows = own_ref.shape[0]
    first = pl.multiple_of(lax.axis_index("actor") * own_rows, own_rows)
    own_ref[...] = w_ref[pl.ds(first, own_rows), :]
    for r in range(0, rows, 16):
        acc = jnp.zeros((16, 128), f32)
        for c in range(0, width, 128):
            x = x_ref[r : r + 16, c : c + 128].astype(f32)
            acc = acc + x * x
        mean = jnp.sum(acc, axis=1, keepdims=True) * (1.0 / width)
        scale = jnp.broadcast_to(lax.rsqrt(mean + 1e-05), (16, 128))
        for c in range(0, width, 128):
            x = x_ref[r : r + 16, c : c + 128].astype(f32)
            n_ref[r : r + 16, c : c + 128] = (x * scale * g_ref[:, c : c + 128]).astype(bf16)
    start = pl.multiple_of(lax.axis_index("mp") * cols, cols)
    local_ref[...] = n_ref[:, pl.ds(start, cols)]
    base_ref[...] = jnp.dot(n_ref[...], w_ref[...], preferred_element_type=f32)


def norm_and_project(resid, gain, weight, own_rows, rows=512):
    tokens, width = resid.shape
    cols = weight.shape[1]
    return pl.pallas_call(
        norm_kernel,
        grid_spec=pltpu.PrefetchScalarGridSpec(
            num_scalar_prefetch=0,
            grid=(tokens // rows,),
            in_specs=[
                pl.BlockSpec((rows, width), lambda i: (i, 0)),
                pl.BlockSpec((width,), lambda i: (0,)),
                pl.BlockSpec((width, cols), lambda i: (0, 0)),
            ],
            out_specs=[
                pl.BlockSpec((rows, cols), lambda i: (i, 0)),
                pl.BlockSpec((rows, cols), lambda i: (i, 0)),
                pl.BlockSpec((own_rows, cols), lambda i: (0, 0)),
            ],
            scratch_shapes=[pltpu.VMEM((rows, width), bf16), pltpu.VMEM((16, width), f32)],
        ),
        out_shape=[
            jax.ShapeDtypeStruct((tokens, cols), f32),
            jax.ShapeDtypeStruct((tokens, cols), bf16),
            jax.ShapeDtypeStruct((own_rows, cols), bf16),
        ],
        compiler_params=pltpu.CompilerParams(vmem_limit_bytes=52 * 2**20),
        cost_estimate=pl.CostEstimate(
            flops=2 * tokens * width * cols,
            bytes_accessed=2 * tokens * width + 2 * width * cols + 6 * tokens * cols,
            transcendentals=0,
        ),
        name="norm_and_project",
    )(resid, gain, weight)


def live_rows(lengths_ref, sequence, shape):
    return lax.broadcasted_iota(jnp.int32, shape, 0) < lengths_ref[sequence]


def half_rows(side, half):
    return pl.ds(pl.multiple_of(side * half, half), half)


def half_products(lengths_ref, table, local_ref, cot_ref, side, out_ref):
    half, lanes = out_ref.shape
    rows = half_rows(side, half)
    swapped = pltpu.roll(table.astype(f32), lanes // 2, 1).astype(bf16)
    back = jnp.dot(cot_ref[rows, :], swapped, preferred_element_type=f32)
    low = jnp.dot(local_ref[rows, :], swapped, preferred_element_type=f32)
    both = jnp.where(lanes_of(back.shape) < lanes // 2, back, low)
    for h in range(half // LEN):
        part = both[h * LEN : (h + 1) * LEN]
        live = live_rows(lengths_ref, side * (half // LEN) + h, part.shape)
        out_ref[h * LEN : (h + 1) * LEN, :] = jnp.where(live, part, 0.0)


def give_kernel(owner_ref, lengths_ref, got_ref, local_ref, cot_ref, table_ref, give_ref):
    blocks, block, lanes = got_ref.shape
    for j in range(blocks):
        table_ref[j * block : (j + 1) * block, :] = got_ref[owner_ref[j]]
    side = 1 - lax.axis_index("mp") % 2
    half_products(lengths_ref, table_ref[...], local_ref, cot_ref, side, give_ref)


def keep_kernel(lengths_ref, table_ref, local_ref, cot_ref, keep_ref):
    side = lax.axis_index("mp") % 2
    half_products(lengths_ref, table_ref[...], local_ref, cot_ref, side, keep_ref)


def whole(n_scalar, n_in, n_out, scratch=()):
    return pltpu.PrefetchScalarGridSpec(
        num_scalar_prefetch=n_scalar,
        grid=(),
        in_specs=[pl.BlockSpec(memory_space=pltpu.VMEM)] * n_in,
        out_specs=[pl.BlockSpec(memory_space=pltpu.VMEM)] * n_out,
        scratch_shapes=list(scratch),
    )


small = pltpu.CompilerParams(vmem_limit_bytes=16 * 2**20)


def cost(flops, moved):
    return pl.CostEstimate(flops=flops, bytes_accessed=moved, transcendentals=0)


def given_products(owner, lengths, got, local, cot):
    lanes = got.shape[2]
    tokens, cols = local.shape
    return pl.pallas_call(
        give_kernel,
        grid_spec=whole(2, 3, 2),
        out_shape=[
            jax.ShapeDtypeStruct((cols, lanes), bf16),
            jax.ShapeDtypeStruct((tokens // 2, lanes), f32),
        ],
        compiler_params=small,
        cost_estimate=cost(2 * tokens * cols * lanes, 2 * tokens * cols + 2 * tokens * lanes),
        name="given_products",
    )(owner, lengths, got, local, cot)


def kept_products(lengths, table, local, cot):
    lanes = table.shape[1]
    tokens, cols = local.shape
    return pl.pallas_call(
        keep_kernel,
        grid_spec=whole(1, 3, 1),
        out_shape=[jax.ShapeDtypeStruct((tokens // 2, lanes), f32)],
        compiler_params=small,
        cost_estimate=cost(2 * tokens * cols * lanes, 2 * tokens * cols + 2 * tokens * lanes),
        name="kept_products",
    )(lengths, table, local, cot)[0]


def half_gradients(rows_ref, side, local_ref, cot_ref):
    half, lanes = rows_ref.shape
    rank = lanes // 2
    rows = half_rows(side, half)
    turned = rows_ref[...].T
    down = jnp.dot(turned[:rank], local_ref[rows, :], preferred_element_type=f32)
    up = jnp.dot(turned[rank:], cot_ref[rows, :], preferred_element_type=f32)
    return jnp.concatenate([down, up], axis=0)


def own_grads_kernel(mine_ref, local_ref, cot_ref, g_ref):
    g_ref[...] = half_gradients(mine_ref, lax.axis_index("mp") % 2, local_ref, cot_ref)


def all_grads_kernel(
    owner_ref, own_ref, mine_ref, other_ref, local_ref, cot_ref, both_ref, sent_ref, g_ref
):
    core = lax.axis_index("mp") % 2
    half = mine_ref.shape[0]
    both_ref[half_rows(core, half), :] = mine_ref[...]
    both_ref[half_rows(1 - core, half), :] = other_ref[...]
    total = own_ref[...] + half_gradients(other_ref, 1 - core, local_ref, cot_ref)
    g_ref[...] = adapter_scale * total.T
    blocks, block, _ = sent_ref.shape
    for j in range(blocks):
        sent_ref[owner_ref[j]] = g_ref[j * block : (j + 1) * block, :].astype(bf16)


def own_gradients(mine, local, cot):
    lanes = mine.shape[1]
    tokens, cols = local.shape
    return pl.pallas_call(
        own_grads_kernel,
        grid_spec=whole(0, 3, 1),
        out_shape=[jax.ShapeDtypeStruct((lanes, cols), f32)],
        compiler_params=small,
        cost_estimate=cost(2 * tokens * cols * lanes, 2 * tokens * cols),
        name="own_gradients",
    )(mine, local, cot)[0]


def gradients(owner, own, mine, other, local, cot):
    lanes = mine.shape[1]
    tokens, cols = local.shape
    blocks = owner.shape[0]
    return pl.pallas_call(
        all_grads_kernel,
        grid_spec=whole(1, 5, 2, [pltpu.VMEM((cols, lanes), f32)]),
        out_shape=[
            jax.ShapeDtypeStruct((tokens, lanes), bf16),
            jax.ShapeDtypeStruct((blocks, cols // blocks, lanes), bf16),
        ],
        compiler_params=small,
        cost_estimate=cost(2 * tokens * cols * lanes, 2 * tokens * cols + 2 * cols * lanes),
        name="gradients",
    )(owner, own, mine, other, local, cot)


def query_kernel(lengths_ref, base_ref, both_ref, table_ref, out_ref, done_ref):
    lanes = both_ref.shape[1]
    table = table_ref[...].astype(f32)
    up = jnp.where(lanes_of(table.shape) >= lanes // 2, table, 0.0).astype(bf16)
    value = base_ref[...] + adapter_scale * dot_nt(both_ref[...], up)
    live = live_rows(lengths_ref, pl.program_id(0), value.shape)
    out_ref[...] = jnp.where(live, value, 0.0).astype(bf16)
    done_ref[...] = jnp.zeros_like(done_ref)


def finished_query(lengths, base, both, table):
    tokens, cols = base.shape
    lanes = both.shape[1]
    return pl.pallas_call(
        query_kernel,
        grid_spec=pltpu.PrefetchScalarGridSpec(
            num_scalar_prefetch=1,
            grid=(tokens // LEN,),
            in_specs=[
                pl.BlockSpec((LEN, cols), lambda i, s: (i, 0)),
                pl.BlockSpec((LEN, lanes), lambda i, s: (i, 0)),
                pl.BlockSpec((cols, lanes), lambda i, s: (0, 0)),
            ],
            out_specs=[
                pl.BlockSpec((LEN, cols), lambda i, s: (i, 0)),
                pl.BlockSpec((16, 128), lambda i, s: (0, 0)),
            ],
        ),
        out_shape=[
            jax.ShapeDtypeStruct((tokens, cols), bf16),
            jax.ShapeDtypeStruct((16, 128), f32),
        ],
        compiler_params=small,
        cost_estimate=cost(2 * tokens * cols * lanes, 6 * tokens * cols),
        name="finished_query",
    )(lengths, base, both, table)


def moved(summed, table, one, two):
    first = beta_one * one + (1.0 - beta_one) * summed
    second = beta_two * two + (1.0 - beta_two) * summed * summed
    updated = table - learn_rate * (first / fix_one) / (jnp.sqrt(second / fix_two) + 1e-08)
    return updated, first, second


def update_kernel(got_ref, done_ref, table_ref, one_ref, two_ref, summed_ref, fresh_ref):
    summed = done_ref[...]
    for j in range(got_ref.shape[0]):
        summed = summed + got_ref[j].astype(f32)
    summed_ref[...] = summed
    fresh_ref[...] = moved(summed, table_ref[...], one_ref[...], two_ref[...])[0].astype(bf16)


def update(got, done, table, one, two):
    return pl.pallas_call(
        update_kernel,
        grid_spec=whole(0, 5, 2),
        out_shape=[
            jax.ShapeDtypeStruct(table.shape, f32),
            jax.ShapeDtypeStruct(table.shape, bf16),
        ],
        compiler_params=small,
        name="update",
    )(got, done, table, one, two)


def offer_kernel(slices_ref, own_ref, out_ref):
    n_mp, block, lanes = slices_ref.shape
    ratio = out_ref.shape[0] // n_mp
    own = own_ref[...].astype(f32)
    for m in range(n_mp):
        down = slices_ref[m].astype(f32)
        value = jnp.where(lanes_of(own.shape) < lanes // 2, down, own).astype(bf16)
        for q in range(ratio):
            out_ref[m * ratio + q] = value


def offered(slices, own, n_actor):
    block, lanes = own.shape
    return pl.pallas_call(
        offer_kernel,
        grid_spec=whole(0, 2, 1),
        out_shape=[jax.ShapeDtypeStruct((n_actor, block, lanes), bf16)],
        compiler_params=small,
        name="offered",
    )(slices, own)[0]


def merge_kernel(
    owner_ref, got_ref, w_ref, summed_ref, table_ref, one_ref, two_ref,
    out_ref, updated_ref, first_ref, second_ref, t_ref,
):
    updated, first, second = moved(summed_ref[...], table_ref[...], one_ref[...], two_ref[...])
    updated_ref[...] = updated
    first_ref[...] = first
    second_ref[...] = second
    blocks, block, lanes = got_ref.shape
    for j in range(blocks):
        t_ref[j * block : (j + 1) * block, :] = got_ref[owner_ref[j]]
    rows = out_ref.shape[0]
    start = pl.multiple_of(lax.axis_index("actor") % (t_ref.shape[0] // rows) * rows, rows)
    down = pltpu.roll(t_ref[pl.ds(start, rows), :].astype(f32), lanes // 2, 1).astype(bf16)
    table = t_ref[...].astype(f32)
    up = jnp.where(lanes_of(table.shape) >= lanes // 2, table, 0.0).astype(bf16)
    out_ref[...] = (w_ref[...].astype(f32) + adapter_scale * dot_nt(down, up)).astype(bf16)


def merge(owner, got, weight_rows, summed, table, one, two):
    blocks, block, lanes = got.shape
    own = jax.ShapeDtypeStruct(table.shape, f32)
    return pl.pallas_call(
        merge_kernel,
        grid_spec=whole(1, 6, 4, [pltpu.VMEM((blocks * block, lanes), bf16)]),
        out_shape=[jax.ShapeDtypeStruct(weight_rows.shape, bf16), own, own, own],
        compiler_params=small,
        name="merge",
    )(owner, got, weight_rows, summed, table, one, two)


def core_swap(x):
    size = lax.axis_size("mp")
    return lax.ppermute(x, "mp", [(i, i ^ 1) for i in range(size)])


def mp_shift(x, k):
    size = lax.axis_size("mp")
    return lax.ppermute(x, "mp", [(i, (i + k) % size) for i in range(size)])


def nearest_first(n):
    return sorted(range(1, n), key=lambda k: min(k, n - k))


def exchanged(x, copies, axis):
    spread = jnp.broadcast_to(x[None], (copies, *x.shape))
    return lax.all_to_all(spread, axis, 0, 0, tiled=True)


def body(
    resid, norm_gain, query_weight, cotangent, lengths, owner, adapter_table, moment_one, moment_two
):
    n_actor = lax.axis_size("actor")
    n_mp = lax.axis_size("mp")
    chips = n_mp // 2
    block = adapter_table.shape[2]
    lanes = adapter_table.shape[3]
    table_now = adapter_table.reshape(block, lanes)
    got = exchanged(table_now.astype(bf16), n_actor, "actor")
    base, local, weight_rows = norm_and_project(
        resid, norm_gain, query_weight, resid.shape[1] // n_actor
    )
    table, give = given_products(owner, lengths, got, local, cotangent)
    own = core_swap(give) + kept_products(lengths, table, local, cotangent)
    sent = own.astype(bf16)
    total = own
    for hops in nearest_first(chips):
        total = total + mp_shift(sent, 2 * hops).astype(f32)
    mine = total.astype(bf16)
    other = core_swap(mine)
    both, grad = gradients(
        owner, own_gradients(mine, local, cotangent), mine, other, local, cotangent
    )
    received = lax.all_to_all(grad, "actor", 0, 0, tiled=True)
    query, done = finished_query(lengths, base, both, table)
    one = moment_one.reshape(block, lanes)
    two = moment_two.reshape(block, lanes)
    summed, fresh = update(received, done, table_now, one, two)
    slices = exchanged(fresh, n_mp, "mp")
    fresh_got = lax.all_to_all(offered(slices, fresh, n_actor), "actor", 0, 0, tiled=True)
    merged, updated, first, second = merge(
        owner, fresh_got, weight_rows, summed, table_now, one, two
    )
    shape = adapter_table.shape
    return (query, updated.reshape(shape), first.reshape(shape), second.reshape(shape), merged)


def solution(mesh):
    return jax.shard_map(
        body,
        mesh=mesh,
        in_specs=(
            P("actor", None),
            P(),
            P(None, "mp"),
            P("actor", "mp"),
            P("actor"),
            P(),
            P("mp", "actor", None, None),
            P("mp", "actor", None, None),
            P("mp", "actor", None, None),
        ),
        out_specs=(
            P("actor", "mp"),
            P("mp", "actor", None, None),
            P("mp", "actor", None, None),
            P("mp", "actor", None, None),
            P("actor", "mp"),
        ),
        check_vma=False,
    )
```

```python
import jax
import jax.numpy as jnp
from jax import lax
from jax.experimental import pallas as pl
from jax.experimental.pallas import tpu as pltpu
from jax.sharding import PartitionSpec as P

LEN = 256


adapter_scale = 0.5
learn_rate = 0.003
beta_one = 0.9
beta_two = 0.999
fix_one = 1.0 - 0.9**10
fix_two = 1.0 - 0.999**10

f32 = jnp.float32
bf16 = jnp.bfloat16


def lanes_of(shape):
    return lax.broadcasted_iota(jnp.int32, shape, 1)


def dot_nt(left, right):
    return lax.dot_general(left, right, (((1,), (1,)), ((), ())), preferred_element_type=f32)


def norm_kernel(x_ref, gain_ref, w_ref, base_ref, local_ref, own_ref, n_ref, g_ref):
    rows, width = x_ref.shape
    cols = base_ref.shape[1]
    g_ref[...] = jnp.broadcast_to(gain_ref[...].astype(f32)[None, :], g_ref.shape)
    own_rows = own_ref.shape[0]
    first = pl.multiple_of(lax.axis_index("actor") * own_rows, own_rows)
    own_ref[...] = w_ref[pl.ds(first, own_rows), :]
    for r in range(0, rows, 16):
        acc = jnp.zeros((16, 128), f32)
        for c in range(0, width, 128):
            x = x_ref[r : r + 16, c : c + 128].astype(f32)
            acc = acc + x * x
        mean = jnp.sum(acc, axis=1, keepdims=True) * (1.0 / width)
        scale = jnp.broadcast_to(lax.rsqrt(mean + 1e-05), (16, 128))
        for c in range(0, width, 128):
            x = x_ref[r : r + 16, c : c + 128].astype(f32)
            n_ref[r : r + 16, c : c + 128] = (x * scale * g_ref[:, c : c + 128]).astype(bf16)
    start = pl.multiple_of(lax.axis_index("mp") * cols, cols)
    local_ref[...] = n_ref[:, pl.ds(start, cols)]
    base_ref[...] = jnp.dot(n_ref[...], w_ref[...], preferred_element_type=f32)


def norm_and_project(resid, gain, weight, own_rows, rows=512):
    tokens, width = resid.shape
    cols = weight.shape[1]
    return pl.pallas_call(
        norm_kernel,
        grid_spec=pltpu.PrefetchScalarGridSpec(
            num_scalar_prefetch=0,
            grid=(tokens // rows,),
            in_specs=[
                pl.BlockSpec((rows, width), lambda i: (i, 0)),
                pl.BlockSpec((width,), lambda i: (0,)),
                pl.BlockSpec((width, cols), lambda i: (0, 0)),
            ],
            out_specs=[
                pl.BlockSpec((rows, cols), lambda i: (i, 0)),
                pl.BlockSpec((rows, cols), lambda i: (i, 0)),
                pl.BlockSpec((own_rows, cols), lambda i: (0, 0)),
            ],
            scratch_shapes=[pltpu.VMEM((rows, width), bf16), pltpu.VMEM((16, width), f32)],
        ),
        out_shape=[
            jax.ShapeDtypeStruct((tokens, cols), f32),
            jax.ShapeDtypeStruct((tokens, cols), bf16),
            jax.ShapeDtypeStruct((own_rows, cols), bf16),
        ],
        compiler_params=pltpu.CompilerParams(vmem_limit_bytes=52 * 2**20),
        cost_estimate=pl.CostEstimate(
            flops=2 * tokens * width * cols,
            bytes_accessed=2 * tokens * width + 2 * width * cols + 6 * tokens * cols,
            transcendentals=0,
        ),
        name="norm_and_project",
    )(resid, gain, weight)


def live_rows(lengths_ref, sequence, shape):
    return lax.broadcasted_iota(jnp.int32, shape, 0) < lengths_ref[sequence]


def half_rows(side, half):
    return pl.ds(pl.multiple_of(side * half, half), half)


def half_products(lengths_ref, table, local_ref, cot_ref, side, out_ref):
    half, lanes = out_ref.shape
    rows = half_rows(side, half)
    swapped = pltpu.roll(table.astype(f32), lanes // 2, 1).astype(bf16)
    back = jnp.dot(cot_ref[rows, :], swapped, preferred_element_type=f32)
    low = jnp.dot(local_ref[rows, :], swapped, preferred_element_type=f32)
    both = jnp.where(lanes_of(back.shape) < lanes // 2, back, low)
    for h in range(half // LEN):
        part = both[h * LEN : (h + 1) * LEN]
        live = live_rows(lengths_ref, side * (half // LEN) + h, part.shape)
        out_ref[h * LEN : (h + 1) * LEN, :] = jnp.where(live, part, 0.0)


def give_kernel(owner_ref, lengths_ref, got_ref, local_ref, cot_ref, table_ref, give_ref):
    blocks, block, lanes = got_ref.shape
    for j in range(blocks):
        table_ref[j * block : (j + 1) * block, :] = got_ref[owner_ref[j]]
    side = 1 - lax.axis_index("mp") % 2
    half_products(lengths_ref, table_ref[...], local_ref, cot_ref, side, give_ref)


def keep_kernel(lengths_ref, table_ref, local_ref, cot_ref, keep_ref):
    side = lax.axis_index("mp") % 2
    half_products(lengths_ref, table_ref[...], local_ref, cot_ref, side, keep_ref)


def whole(n_scalar, n_in, n_out, scratch=()):
    return pltpu.PrefetchScalarGridSpec(
        num_scalar_prefetch=n_scalar,
        grid=(),
        in_specs=[pl.BlockSpec(memory_space=pltpu.VMEM)] * n_in,
        out_specs=[pl.BlockSpec(memory_space=pltpu.VMEM)] * n_out,
        scratch_shapes=list(scratch),
    )


small = pltpu.CompilerParams(vmem_limit_bytes=16 * 2**20)


def cost(flops, moved):
    return pl.CostEstimate(flops=flops, bytes_accessed=moved, transcendentals=0)


def given_products(owner, lengths, got, local, cot):
    lanes = got.shape[2]
    tokens, cols = local.shape
    return pl.pallas_call(
        give_kernel,
        grid_spec=whole(2, 3, 2),
        out_shape=[
            jax.ShapeDtypeStruct((cols, lanes), bf16),
            jax.ShapeDtypeStruct((tokens // 2, lanes), f32),
        ],
        compiler_params=small,
        cost_estimate=cost(2 * tokens * cols * lanes, 2 * tokens * cols + 2 * tokens * lanes),
        name="given_products",
    )(owner, lengths, got, local, cot)


def kept_products(lengths, table, local, cot):
    lanes = table.shape[1]
    tokens, cols = local.shape
    return pl.pallas_call(
        keep_kernel,
        grid_spec=whole(1, 3, 1),
        out_shape=[jax.ShapeDtypeStruct((tokens // 2, lanes), f32)],
        compiler_params=small,
        cost_estimate=cost(2 * tokens * cols * lanes, 2 * tokens * cols + 2 * tokens * lanes),
        name="kept_products",
    )(lengths, table, local, cot)[0]


def half_gradients(rows_ref, side, local_ref, cot_ref):
    half, lanes = rows_ref.shape
    rank = lanes // 2
    rows = half_rows(side, half)
    turned = rows_ref[...].T
    down = jnp.dot(turned[:rank], local_ref[rows, :], preferred_element_type=f32)
    up = jnp.dot(turned[rank:], cot_ref[rows, :], preferred_element_type=f32)
    return jnp.concatenate([down, up], axis=0)


def own_grads_kernel(mine_ref, local_ref, cot_ref, g_ref):
    g_ref[...] = half_gradients(mine_ref, lax.axis_index("mp") % 2, local_ref, cot_ref)


def all_grads_kernel(
    owner_ref, own_ref, mine_ref, other_ref, local_ref, cot_ref, both_ref, sent_ref, g_ref
):
    core = lax.axis_index("mp") % 2
    half = mine_ref.shape[0]
    both_ref[half_rows(core, half), :] = mine_ref[...]
    both_ref[half_rows(1 - core, half), :] = other_ref[...]
    total = own_ref[...] + half_gradients(other_ref, 1 - core, local_ref, cot_ref)
    g_ref[...] = adapter_scale * total.T
    blocks, block, _ = sent_ref.shape
    for j in range(blocks):
        sent_ref[owner_ref[j]] = g_ref[j * block : (j + 1) * block, :].astype(bf16)


def own_gradients(mine, local, cot):
    lanes = mine.shape[1]
    tokens, cols = local.shape
    return pl.pallas_call(
        own_grads_kernel,
        grid_spec=whole(0, 3, 1),
        out_shape=[jax.ShapeDtypeStruct((lanes, cols), f32)],
        compiler_params=small,
        cost_estimate=cost(2 * tokens * cols * lanes, 2 * tokens * cols),
        name="own_gradients",
    )(mine, local, cot)[0]


def gradients(owner, own, mine, other, local, cot):
    lanes = mine.shape[1]
    tokens, cols = local.shape
    blocks = owner.shape[0]
    return pl.pallas_call(
        all_grads_kernel,
        grid_spec=whole(1, 5, 2, [pltpu.VMEM((cols, lanes), f32)]),
        out_shape=[
            jax.ShapeDtypeStruct((tokens, lanes), bf16),
            jax.ShapeDtypeStruct((blocks, cols // blocks, lanes), bf16),
        ],
        compiler_params=small,
        cost_estimate=cost(2 * tokens * cols * lanes, 2 * tokens * cols + 2 * cols * lanes),
        name="gradients",
    )(owner, own, mine, other, local, cot)


def query_kernel(lengths_ref, base_ref, both_ref, table_ref, out_ref, done_ref):
    lanes = both_ref.shape[1]
    table = table_ref[...].astype(f32)
    up = jnp.where(lanes_of(table.shape) >= lanes // 2, table, 0.0).astype(bf16)
    value = base_ref[...] + adapter_scale * dot_nt(both_ref[...], up)
    live = live_rows(lengths_ref, pl.program_id(0), value.shape)
    out_ref[...] = jnp.where(live, value, 0.0).astype(bf16)
    done_ref[...] = jnp.zeros_like(done_ref)


def finished_query(lengths, base, both, table):
    tokens, cols = base.shape
    lanes = both.shape[1]
    return pl.pallas_call(
        query_kernel,
        grid_spec=pltpu.PrefetchScalarGridSpec(
            num_scalar_prefetch=1,
            grid=(tokens // LEN,),
            in_specs=[
                pl.BlockSpec((LEN, cols), lambda i, s: (i, 0)),
                pl.BlockSpec((LEN, lanes), lambda i, s: (i, 0)),
                pl.BlockSpec((cols, lanes), lambda i, s: (0, 0)),
            ],
            out_specs=[
                pl.BlockSpec((LEN, cols), lambda i, s: (i, 0)),
                pl.BlockSpec((16, 128), lambda i, s: (0, 0)),
            ],
        ),
        out_shape=[
            jax.ShapeDtypeStruct((tokens, cols), bf16),
            jax.ShapeDtypeStruct((16, 128), f32),
        ],
        compiler_params=small,
        cost_estimate=cost(2 * tokens * cols * lanes, 6 * tokens * cols),
        name="finished_query",
    )(lengths, base, both, table)


def moved(summed, table, one, two):
    first = beta_one * one + (1.0 - beta_one) * summed
    second = beta_two * two + (1.0 - beta_two) * summed * summed
    updated = table - learn_rate * (first / fix_one) / (jnp.sqrt(second / fix_two) + 1e-08)
    return updated, first, second


def update_kernel(got_ref, done_ref, table_ref, one_ref, two_ref, summed_ref, fresh_ref):
    summed = done_ref[...]
    for j in range(got_ref.shape[0]):
        summed = summed + got_ref[j].astype(f32)
    summed_ref[...] = summed
    fresh_ref[...] = moved(summed, table_ref[...], one_ref[...], two_ref[...])[0].astype(bf16)


def update(got, done, table, one, two):
    return pl.pallas_call(
        update_kernel,
        grid_spec=whole(0, 5, 2),
        out_shape=[
            jax.ShapeDtypeStruct(table.shape, f32),
            jax.ShapeDtypeStruct(table.shape, bf16),
        ],
        compiler_params=small,
        name="update",
    )(got, done, table, one, two)


def offer_kernel(slices_ref, own_ref, out_ref):
    n_mp, block, lanes = slices_ref.shape
    ratio = out_ref.shape[0] // n_mp
    own = own_ref[...].astype(f32)
    for m in range(n_mp):
        down = slices_ref[m].astype(f32)
        value = jnp.where(lanes_of(own.shape) < lanes // 2, down, own).astype(bf16)
        for q in range(ratio):
            out_ref[m * ratio + q] = value


def offered(slices, own, n_actor):
    block, lanes = own.shape
    return pl.pallas_call(
        offer_kernel,
        grid_spec=whole(0, 2, 1),
        out_shape=[jax.ShapeDtypeStruct((n_actor, block, lanes), bf16)],
        compiler_params=small,
        name="offered",
    )(slices, own)[0]


def merge_kernel(
    owner_ref, got_ref, w_ref, summed_ref, table_ref, one_ref, two_ref,
    out_ref, updated_ref, first_ref, second_ref, t_ref,
):
    updated, first, second = moved(summed_ref[...], table_ref[...], one_ref[...], two_ref[...])
    updated_ref[...] = updated
    first_ref[...] = first
    second_ref[...] = second
    blocks, block, lanes = got_ref.shape
    for j in range(blocks):
        t_ref[j * block : (j + 1) * block, :] = got_ref[owner_ref[j]]
    rows = out_ref.shape[0]
    start = pl.multiple_of(lax.axis_index("actor") % (t_ref.shape[0] // rows) * rows, rows)
    down = pltpu.roll(t_ref[pl.ds(start, rows), :].astype(f32), lanes // 2, 1).astype(bf16)
    table = t_ref[...].astype(f32)
    up = jnp.where(lanes_of(table.shape) >= lanes // 2, table, 0.0).astype(bf16)
    out_ref[...] = (w_ref[...].astype(f32) + adapter_scale * dot_nt(down, up)).astype(bf16)


def merge(owner, got, weight_rows, summed, table, one, two):
    blocks, block, lanes = got.shape
    own = jax.ShapeDtypeStruct(table.shape, f32)
    return pl.pallas_call(
        merge_kernel,
        grid_spec=whole(1, 6, 4, [pltpu.VMEM((blocks * block, lanes), bf16)]),
        out_shape=[jax.ShapeDtypeStruct(weight_rows.shape, bf16), own, own, own],
        compiler_params=small,
        name="merge",
    )(owner, got, weight_rows, summed, table, one, two)


def core_swap(x):
    size = lax.axis_size("mp")
    return lax.ppermute(x, "mp", [(i, i ^ 1) for i in range(size)])


def mp_shift(x, k):
    size = lax.axis_size("mp")
    return lax.ppermute(x, "mp", [(i, (i + k) % size) for i in range(size)])


def nearest_first(n):
    return sorted(range(1, n), key=lambda k: (min(k, n - k), -k))


def exchanged(x, copies, axis):
    spread = jnp.broadcast_to(x[None], (copies, *x.shape))
    return lax.all_to_all(spread, axis, 0, 0, tiled=True)


def body(
    resid, norm_gain, query_weight, cotangent, lengths, owner, adapter_table, moment_one, moment_two
):
    n_actor = lax.axis_size("actor")
    n_mp = lax.axis_size("mp")
    chips = n_mp // 2
    block = adapter_table.shape[2]
    lanes = adapter_table.shape[3]
    table_now = adapter_table.reshape(block, lanes)
    got = exchanged(table_now.astype(bf16), n_actor, "actor")
    base, local, weight_rows = norm_and_project(
        resid, norm_gain, query_weight, resid.shape[1] // n_actor
    )
    table, give = given_products(owner, lengths, got, local, cotangent)
    own = core_swap(give) + kept_products(lengths, table, local, cotangent)
    sent = own.astype(bf16)
    total = own
    for hops in nearest_first(chips):
        total = total + mp_shift(sent, 2 * hops).astype(f32)
    mine = total.astype(bf16)
    other = core_swap(mine)
    both, grad = gradients(
        owner, own_gradients(mine, local, cotangent), mine, other, local, cotangent
    )
    received = lax.all_to_all(grad, "actor", 0, 0, tiled=True)
    query, done = finished_query(lengths, base, both, table)
    one = moment_one.reshape(block, lanes)
    two = moment_two.reshape(block, lanes)
    summed, fresh = update(received, done, table_now, one, two)
    slices = exchanged(fresh, n_mp, "mp")
    fresh_got = lax.all_to_all(offered(slices, fresh, n_actor), "actor", 0, 0, tiled=True)
    merged, updated, first, second = merge(
        owner, fresh_got, weight_rows, summed, table_now, one, two
    )
    shape = adapter_table.shape
    return (query, updated.reshape(shape), first.reshape(shape), second.reshape(shape), merged)


def solution(mesh):
    return jax.shard_map(
        body,
        mesh=mesh,
        in_specs=(
            P("actor", None),
            P(),
            P(None, "mp"),
            P("actor", "mp"),
            P("actor"),
            P(),
            P("mp", "actor", None, None),
            P("mp", "actor", None, None),
            P("mp", "actor", None, None),
        ),
        out_specs=(
            P("actor", "mp"),
            P("mp", "actor", None, None),
            P("mp", "actor", None, None),
            P("mp", "actor", None, None),
            P("actor", "mp"),
        ),
        check_vma=False,
    )
```

```python
import jax
import jax.numpy as jnp
from jax import lax
from jax.experimental import pallas as pl
from jax.experimental.pallas import tpu as pltpu
from jax.sharding import PartitionSpec as P

LEN = 256


adapter_scale = 0.5
learn_rate = 0.003
beta_one = 0.9
beta_two = 0.999
fix_one = 1.0 - 0.9**10
fix_two = 1.0 - 0.999**10

f32 = jnp.float32
bf16 = jnp.bfloat16


def lanes_of(shape):
    return lax.broadcasted_iota(jnp.int32, shape, 1)


def dot_nt(left, right):
    return lax.dot_general(left, right, (((1,), (1,)), ((), ())), preferred_element_type=f32)


def norm_kernel(x_ref, gain_ref, w_ref, base_ref, local_ref, own_ref, n_ref, g_ref):
    rows, width = x_ref.shape
    cols = base_ref.shape[1]
    g_ref[...] = jnp.broadcast_to(gain_ref[...].astype(f32)[None, :], g_ref.shape)
    own_rows = own_ref.shape[0]
    first = pl.multiple_of(lax.axis_index("actor") * own_rows, own_rows)
    own_ref[...] = w_ref[pl.ds(first, own_rows), :]
    for r in range(0, rows, 16):
        acc = jnp.zeros((16, 128), f32)
        for c in range(0, width, 128):
            x = x_ref[r : r + 16, c : c + 128].astype(f32)
            acc = acc + x * x
        mean = jnp.sum(acc, axis=1, keepdims=True) * (1.0 / width)
        scale = jnp.broadcast_to(lax.rsqrt(mean + 1e-05), (16, 128))
        for c in range(0, width, 128):
            x = x_ref[r : r + 16, c : c + 128].astype(f32)
            n_ref[r : r + 16, c : c + 128] = (x * scale * g_ref[:, c : c + 128]).astype(bf16)
    start = pl.multiple_of(lax.axis_index("mp") * cols, cols)
    local_ref[...] = n_ref[:, pl.ds(start, cols)]
    base_ref[...] = jnp.dot(n_ref[...], w_ref[...], preferred_element_type=f32)


def norm_and_project(resid, gain, weight, own_rows, rows=512):
    tokens, width = resid.shape
    cols = weight.shape[1]
    return pl.pallas_call(
        norm_kernel,
        grid_spec=pltpu.PrefetchScalarGridSpec(
            num_scalar_prefetch=0,
            grid=(tokens // rows,),
            in_specs=[
                pl.BlockSpec((rows, width), lambda i: (i, 0)),
                pl.BlockSpec((width,), lambda i: (0,)),
                pl.BlockSpec((width, cols), lambda i: (0, 0)),
            ],
            out_specs=[
                pl.BlockSpec((rows, cols), lambda i: (i, 0)),
                pl.BlockSpec((rows, cols), lambda i: (i, 0)),
                pl.BlockSpec((own_rows, cols), lambda i: (0, 0)),
            ],
            scratch_shapes=[pltpu.VMEM((rows, width), bf16), pltpu.VMEM((16, width), f32)],
        ),
        out_shape=[
            jax.ShapeDtypeStruct((tokens, cols), f32),
            jax.ShapeDtypeStruct((tokens, cols), bf16),
            jax.ShapeDtypeStruct((own_rows, cols), bf16),
        ],
        compiler_params=pltpu.CompilerParams(vmem_limit_bytes=52 * 2**20),
        cost_estimate=pl.CostEstimate(
            flops=2 * tokens * width * cols,
            bytes_accessed=2 * tokens * width + 2 * width * cols + 6 * tokens * cols,
            transcendentals=0,
        ),
        name="norm_and_project",
    )(resid, gain, weight)


def live_rows(lengths_ref, sequence, shape):
    return lax.broadcasted_iota(jnp.int32, shape, 0) < lengths_ref[sequence]


def half_rows(side, half):
    return pl.ds(pl.multiple_of(side * half, half), half)


def half_products(lengths_ref, table, local_ref, cot_ref, side, out_ref):
    half, lanes = out_ref.shape
    rows = half_rows(side, half)
    swapped = pltpu.roll(table.astype(f32), lanes // 2, 1).astype(bf16)
    back = jnp.dot(cot_ref[rows, :], swapped, preferred_element_type=f32)
    low = jnp.dot(local_ref[rows, :], swapped, preferred_element_type=f32)
    both = jnp.where(lanes_of(back.shape) < lanes // 2, back, low)
    for h in range(half // LEN):
        part = both[h * LEN : (h + 1) * LEN]
        live = live_rows(lengths_ref, side * (half // LEN) + h, part.shape)
        out_ref[h * LEN : (h + 1) * LEN, :] = jnp.where(live, part, 0.0)


def give_kernel(owner_ref, lengths_ref, got_ref, local_ref, cot_ref, table_ref, give_ref):
    blocks, block, lanes = got_ref.shape
    for j in range(blocks):
        table_ref[j * block : (j + 1) * block, :] = got_ref[owner_ref[j]]
    side = 1 - lax.axis_index("mp") % 2
    half_products(lengths_ref, table_ref[...], local_ref, cot_ref, side, give_ref)


def keep_kernel(lengths_ref, table_ref, local_ref, cot_ref, keep_ref):
    side = lax.axis_index("mp") % 2
    half_products(lengths_ref, table_ref[...], local_ref, cot_ref, side, keep_ref)


def whole(n_scalar, n_in, n_out, scratch=()):
    return pltpu.PrefetchScalarGridSpec(
        num_scalar_prefetch=n_scalar,
        grid=(),
        in_specs=[pl.BlockSpec(memory_space=pltpu.VMEM)] * n_in,
        out_specs=[pl.BlockSpec(memory_space=pltpu.VMEM)] * n_out,
        scratch_shapes=list(scratch),
    )


small = pltpu.CompilerParams(vmem_limit_bytes=16 * 2**20)


def cost(flops, moved):
    return pl.CostEstimate(flops=flops, bytes_accessed=moved, transcendentals=0)


def given_products(owner, lengths, got, local, cot):
    lanes = got.shape[2]
    tokens, cols = local.shape
    return pl.pallas_call(
        give_kernel,
        grid_spec=whole(2, 3, 2),
        out_shape=[
            jax.ShapeDtypeStruct((cols, lanes), bf16),
            jax.ShapeDtypeStruct((tokens // 2, lanes), f32),
        ],
        compiler_params=small,
        cost_estimate=cost(2 * tokens * cols * lanes, 2 * tokens * cols + 2 * tokens * lanes),
        name="given_products",
    )(owner, lengths, got, local, cot)


def kept_products(lengths, table, local, cot):
    lanes = table.shape[1]
    tokens, cols = local.shape
    return pl.pallas_call(
        keep_kernel,
        grid_spec=whole(1, 3, 1),
        out_shape=[jax.ShapeDtypeStruct((tokens // 2, lanes), f32)],
        compiler_params=small,
        cost_estimate=cost(2 * tokens * cols * lanes, 2 * tokens * cols + 2 * tokens * lanes),
        name="kept_products",
    )(lengths, table, local, cot)[0]


def half_gradients(rows_ref, side, local_ref, cot_ref):
    half, lanes = rows_ref.shape
    rank = lanes // 2
    rows = half_rows(side, half)
    turned = rows_ref[...].T
    down = jnp.dot(turned[:rank], local_ref[rows, :], preferred_element_type=f32)
    up = jnp.dot(turned[rank:], cot_ref[rows, :], preferred_element_type=f32)
    return jnp.concatenate([down, up], axis=0)


def own_grads_kernel(mine_ref, local_ref, cot_ref, g_ref):
    g_ref[...] = half_gradients(mine_ref, lax.axis_index("mp") % 2, local_ref, cot_ref)


def all_grads_kernel(
    owner_ref, own_ref, mine_ref, other_ref, local_ref, cot_ref, both_ref, sent_ref, g_ref
):
    core = lax.axis_index("mp") % 2
    half = mine_ref.shape[0]
    both_ref[half_rows(core, half), :] = mine_ref[...]
    both_ref[half_rows(1 - core, half), :] = other_ref[...]
    total = own_ref[...] + half_gradients(other_ref, 1 - core, local_ref, cot_ref)
    g_ref[...] = adapter_scale * total.T
    blocks, block, _ = sent_ref.shape
    for j in range(blocks):
        sent_ref[owner_ref[j]] = g_ref[j * block : (j + 1) * block, :].astype(bf16)


def own_gradients(mine, local, cot):
    lanes = mine.shape[1]
    tokens, cols = local.shape
    return pl.pallas_call(
        own_grads_kernel,
        grid_spec=whole(0, 3, 1),
        out_shape=[jax.ShapeDtypeStruct((lanes, cols), f32)],
        compiler_params=small,
        cost_estimate=cost(2 * tokens * cols * lanes, 2 * tokens * cols),
        name="own_gradients",
    )(mine, local, cot)[0]


def gradients(owner, own, mine, other, local, cot):
    lanes = mine.shape[1]
    tokens, cols = local.shape
    blocks = owner.shape[0]
    return pl.pallas_call(
        all_grads_kernel,
        grid_spec=whole(1, 5, 2, [pltpu.VMEM((cols, lanes), f32)]),
        out_shape=[
            jax.ShapeDtypeStruct((tokens, lanes), bf16),
            jax.ShapeDtypeStruct((blocks, cols // blocks, lanes), bf16),
        ],
        compiler_params=small,
        cost_estimate=cost(2 * tokens * cols * lanes, 2 * tokens * cols + 2 * cols * lanes),
        name="gradients",
    )(owner, own, mine, other, local, cot)


def query_kernel(lengths_ref, base_ref, both_ref, table_ref, out_ref, done_ref):
    lanes = both_ref.shape[1]
    table = table_ref[...].astype(f32)
    up = jnp.where(lanes_of(table.shape) >= lanes // 2, table, 0.0).astype(bf16)
    value = base_ref[...] + adapter_scale * dot_nt(both_ref[...], up)
    live = live_rows(lengths_ref, pl.program_id(0), value.shape)
    out_ref[...] = jnp.where(live, value, 0.0).astype(bf16)
    done_ref[...] = jnp.zeros_like(done_ref)


def finished_query(lengths, base, both, table):
    tokens, cols = base.shape
    lanes = both.shape[1]
    return pl.pallas_call(
        query_kernel,
        grid_spec=pltpu.PrefetchScalarGridSpec(
            num_scalar_prefetch=1,
            grid=(tokens // LEN,),
            in_specs=[
                pl.BlockSpec((LEN, cols), lambda i, s: (i, 0)),
                pl.BlockSpec((LEN, lanes), lambda i, s: (i, 0)),
                pl.BlockSpec((cols, lanes), lambda i, s: (0, 0)),
            ],
            out_specs=[
                pl.BlockSpec((LEN, cols), lambda i, s: (i, 0)),
                pl.BlockSpec((16, 128), lambda i, s: (0, 0)),
            ],
        ),
        out_shape=[
            jax.ShapeDtypeStruct((tokens, cols), bf16),
            jax.ShapeDtypeStruct((16, 128), f32),
        ],
        compiler_params=small,
        cost_estimate=cost(2 * tokens * cols * lanes, 6 * tokens * cols),
        name="finished_query",
    )(lengths, base, both, table)


def moved(summed, table, one, two):
    first = beta_one * one + (1.0 - beta_one) * summed
    second = beta_two * two + (1.0 - beta_two) * summed * summed
    updated = table - learn_rate * (first / fix_one) / (jnp.sqrt(second / fix_two) + 1e-08)
    return updated, first, second


def update_kernel(got_ref, done_ref, table_ref, one_ref, two_ref, summed_ref, fresh_ref):
    summed = done_ref[...]
    for j in range(got_ref.shape[0]):
        summed = summed + got_ref[j].astype(f32)
    summed_ref[...] = summed
    fresh_ref[...] = moved(summed, table_ref[...], one_ref[...], two_ref[...])[0].astype(bf16)


def update(got, done, table, one, two):
    return pl.pallas_call(
        update_kernel,
        grid_spec=whole(0, 5, 2),
        out_shape=[
            jax.ShapeDtypeStruct(table.shape, f32),
            jax.ShapeDtypeStruct(table.shape, bf16),
        ],
        compiler_params=small,
        name="update",
    )(got, done, table, one, two)


def offer_kernel(slices_ref, own_ref, out_ref):
    n_mp, block, lanes = slices_ref.shape
    ratio = out_ref.shape[0] // n_mp
    own = own_ref[...].astype(f32)
    for m in range(n_mp):
        down = slices_ref[m].astype(f32)
        value = jnp.where(lanes_of(own.shape) < lanes // 2, down, own).astype(bf16)
        for q in range(ratio):
            out_ref[m * ratio + q] = value


def offered(slices, own, n_actor):
    block, lanes = own.shape
    return pl.pallas_call(
        offer_kernel,
        grid_spec=whole(0, 2, 1),
        out_shape=[jax.ShapeDtypeStruct((n_actor, block, lanes), bf16)],
        compiler_params=small,
        name="offered",
    )(slices, own)[0]


def merge_kernel(
    owner_ref, got_ref, w_ref, summed_ref, table_ref, one_ref, two_ref,
    out_ref, updated_ref, first_ref, second_ref, t_ref,
):
    updated, first, second = moved(summed_ref[...], table_ref[...], one_ref[...], two_ref[...])
    updated_ref[...] = updated
    first_ref[...] = first
    second_ref[...] = second
    blocks, block, lanes = got_ref.shape
    for j in range(blocks):
        t_ref[j * block : (j + 1) * block, :] = got_ref[owner_ref[j]]
    rows = out_ref.shape[0]
    start = pl.multiple_of(lax.axis_index("actor") % (t_ref.shape[0] // rows) * rows, rows)
    down = pltpu.roll(t_ref[pl.ds(start, rows), :].astype(f32), lanes // 2, 1)
    down = jnp.where(lanes_of(down.shape) >= lanes // 2, down, 0.0).astype(bf16)
    product = dot_nt(down, t_ref[...])
    out_ref[...] = (w_ref[...].astype(f32) + adapter_scale * product).astype(bf16)


def merge(owner, got, weight_rows, summed, table, one, two):
    blocks, block, lanes = got.shape
    own = jax.ShapeDtypeStruct(table.shape, f32)
    return pl.pallas_call(
        merge_kernel,
        grid_spec=whole(1, 6, 4, [pltpu.VMEM((blocks * block, lanes), bf16)]),
        out_shape=[jax.ShapeDtypeStruct(weight_rows.shape, bf16), own, own, own],
        compiler_params=small,
        name="merge",
    )(owner, got, weight_rows, summed, table, one, two)


def core_swap(x):
    size = lax.axis_size("mp")
    return lax.ppermute(x, "mp", [(i, i ^ 1) for i in range(size)])


def mp_shift(x, k):
    size = lax.axis_size("mp")
    return lax.ppermute(x, "mp", [(i, (i + k) % size) for i in range(size)])


def nearest_first(n):
    return sorted(range(1, n), key=lambda k: (min(k, n - k), -k))


def exchanged(x, copies, axis):
    spread = jnp.broadcast_to(x[None], (copies, *x.shape))
    return lax.all_to_all(spread, axis, 0, 0, tiled=True)


def body(
    resid, norm_gain, query_weight, cotangent, lengths, owner, adapter_table, moment_one, moment_two
):
    n_actor = lax.axis_size("actor")
    n_mp = lax.axis_size("mp")
    chips = n_mp // 2
    block = adapter_table.shape[2]
    lanes = adapter_table.shape[3]
    table_now = adapter_table.reshape(block, lanes)
    got = exchanged(table_now.astype(bf16), n_actor, "actor")
    base, local, weight_rows = norm_and_project(
        resid, norm_gain, query_weight, resid.shape[1] // n_actor
    )
    table, give = given_products(owner, lengths, got, local, cotangent)
    own = core_swap(give) + kept_products(lengths, table, local, cotangent)
    sent = own.astype(bf16)
    total = own
    for hops in nearest_first(chips):
        total = total + mp_shift(sent, 2 * hops).astype(f32)
    mine = total.astype(bf16)
    other = core_swap(mine)
    both, grad = gradients(
        owner, own_gradients(mine, local, cotangent), mine, other, local, cotangent
    )
    received = lax.all_to_all(grad, "actor", 0, 0, tiled=True)
    query, done = finished_query(lengths, base, both, table)
    one = moment_one.reshape(block, lanes)
    two = moment_two.reshape(block, lanes)
    summed, fresh = update(received, done, table_now, one, two)
    slices = exchanged(fresh, n_mp, "mp")
    fresh_got = lax.all_to_all(offered(slices, fresh, n_actor), "actor", 0, 0, tiled=True)
    merged, updated, first, second = merge(
        owner, fresh_got, weight_rows, summed, table_now, one, two
    )
    shape = adapter_table.shape
    return (query, updated.reshape(shape), first.reshape(shape), second.reshape(shape), merged)


def solution(mesh):
    return jax.shard_map(
        body,
        mesh=mesh,
        in_specs=(
            P("actor", None),
            P(),
            P(None, "mp"),
            P("actor", "mp"),
            P("actor"),
            P(),
            P("mp", "actor", None, None),
            P("mp", "actor", None, None),
            P("mp", "actor", None, None),
        ),
        out_specs=(
            P("actor", "mp"),
            P("mp", "actor", None, None),
            P("mp", "actor", None, None),
            P("mp", "actor", None, None),
            P("actor", "mp"),
        ),
        check_vma=False,
    )
```
